32 devices in a mesh: blk: 16 (over z, y, x), uly: 2 (over core).
Axes of the slice: x: 2, y: 2, z: 4, core: 2. Of those that a mesh axis runs over, the one named last changes fastest.
Arguments:
- queries: bfloat16 [3072, 8192], P(('blk', 'uly')), may hold values from -300 to 300
- keys: bfloat16 [3072, 1024], P(('blk', 'uly')), may hold values from -4 to 4
- values: bfloat16 [3072, 1024], P(('blk', 'uly')), may hold values from -6 to 6
- doc_lengths: int32 [32], replicated, may hold values from 1 to 384, as said below
Outputs:
- attention: bfloat16 [3072, 8192], P(('blk', 'uly'))
The draws below stay inside these ranges and needn't reach their ends.
Inputs may be any that keep to these rules, and one draw needn't show every extreme that they name: `doc_lengths`: every document has 1 to 384 tokens, the lengths sum to 3072, and some document has exactly 384 tokens.
All inputs are finite; a program needn't handle non-finite values.
Results may differ from the reference program's by a relative error of at most 0.003.
Values may be sent and summed in bfloat16 or wider, within the bound.
No kernel may reach another device: no remote copies, remote signals or barrier semaphores. Data moves between devices by JAX's collectives and lax.ppermute only.
A program may use at most 64 MiB of HBM per device.

```python
import jax
import jax.numpy as jnp
from jax import lax

HEADS = 64
KV_HEADS = 8
HEAD_DIM = 128
TOK_DEV = 96
REACH = 2
BLOCK = 192
SEQ = 3072
MOST = 384
DOCS = 32
N_BLK = 16
N_ULY = 2


def paired(key):
    base_key = jax.random.fold_in(key, 11)
    first_key, second_key = jax.random.split(base_key, 2)
    width_keys = KV_HEADS * HEAD_DIM
    width_queries = HEADS * HEAD_DIM
    keys_drawn = jax.random.truncated_normal(first_key, -4.0, 4.0, (SEQ, width_keys), jnp.float32)
    queries_drawn = jax.random.truncated_normal(second_key, -4.0, 4.0, (SEQ, width_queries), jnp.float32)
    return (queries_drawn, keys_drawn)


def draw_queries(key, part):
    return paired(key)[0].astype(jnp.bfloat16)


def draw_keys(key, part):
    return paired(key)[1].astype(jnp.bfloat16)


def draw_doc_lengths(key, part):
    offset_key, rank_key = jax.random.split(jax.random.fold_in(key, 23))
    opening = BLOCK // 2
    remaining = SEQ - opening - MOST
    stride = MOST // 2
    candidates = remaining - 1
    strata = (candidates + stride - 1) // stride
    stratum_ids = jnp.arange(strata, dtype=jnp.int32)
    limits = jnp.minimum(stride, candidates - stratum_ids * stride).astype(jnp.int32)
    offsets = jax.random.randint(offset_key, (strata,), 0, limits).astype(jnp.int32)
    positions = jnp.arange(candidates, dtype=jnp.int32)
    forced = (positions % stride == offsets[positions // stride]).astype(jnp.int32)
    ranks = jax.random.permutation(rank_key, candidates).astype(jnp.int32)
    score = forced * candidates + ranks
    order = jnp.argsort(-score, stable=True)[:DOCS - 3].astype(jnp.int32)
    cuts = jnp.sort(order + 1).astype(jnp.int32)
    bounds = jnp.concatenate([jnp.zeros((1,), jnp.int32), cuts, jnp.full((1,), remaining, jnp.int32)])
    gaps = (bounds[1:] - bounds[:-1]).astype(jnp.int32)
    leading = jnp.array([opening, MOST], jnp.int32)
    return jnp.concatenate([leading, gaps]).astype(jnp.int32)


def block_levels(stream_key, shape, shards, smallest, largest):
    factor_of, own = 1.0, jax.random.fold_in(stream_key, 6)
    for axis_at, blocks in shards:
        heights = jnp.exp(jax.random.uniform(jax.random.fold_in(own, axis_at), (blocks,), jnp.float32, smallest / len(shards), largest / len(shards)))
        factor_of = factor_of * jnp.repeat(heights, shape[axis_at] // blocks).reshape([-1 if axis == axis_at else 1 for axis in range(len(shape))])
    return factor_of


def gaussian(rng, shape, spread, limit, pieces=(), kind=jnp.bfloat16):
    gain = block_levels(rng, shape, pieces, -0.22, 0.18) if pieces else 1.0
    drawn = jax.random.normal(rng, shape, jnp.float32) * spread * gain
    return jnp.minimum(jnp.maximum(drawn, -limit), limit).astype(kind)


def setup_inputs(seed: int = 0) -> dict:
    splits = jax.random.split(jax.random.key(seed), 5)
    queries = draw_queries(jax.random.fold_in(splits[4], 71), 0)
    keys = draw_keys(jax.random.fold_in(splits[4], 71), 0)
    values = gaussian(splits[2], (SEQ, KV_HEADS * HEAD_DIM), 1.0, 6.0, ((0, 32),))
    doc_lengths = draw_doc_lengths(jax.random.fold_in(splits[4], 71), 0)
    return dict(queries=queries, keys=keys, values=values, doc_lengths=doc_lengths)


MASKED = -1e30


def doc_index(positions, starts):
    return jnp.sum((positions[:, None] >= starts[None, :]).astype(jnp.int32), axis=1).astype(jnp.int32) - 1


def fold_block(running, grouped, query_pos, query_doc, key_block, value_block, anchor, starts):
    block_rows = key_block.shape[0]
    running_max, row_total, weighted = running
    key_pos = anchor * block_rows + jnp.arange(block_rows, dtype=jnp.int32)
    key_doc = doc_index(key_pos, starts)
    allowed = (key_doc[None, :] == query_doc[:, None]) & (key_pos[None, :] <= query_pos[:, None])
    heads_kv = key_block.shape[1] // HEAD_DIM
    key_heads = key_block.reshape(block_rows, heads_kv, HEAD_DIM).transpose(1, 0, 2).astype(jnp.float32)
    value_heads = value_block.reshape(block_rows, heads_kv, HEAD_DIM).transpose(1, 0, 2).astype(jnp.float32)
    scores = jnp.einsum("gqd,gkd->gqk", grouped.astype(jnp.float32), key_heads) * (HEAD_DIM ** -0.5)
    scores = jnp.where(allowed[None], scores, jnp.float32(MASKED))
    new_max = jnp.maximum(running_max, jnp.max(scores, axis=-1))
    rescale = jnp.exp(running_max - new_max)
    weights = jnp.exp(scores - new_max[..., None])
    row_total = row_total * rescale + jnp.sum(weights, axis=-1)
    rounded = lax.optimization_barrier(weights.astype(jnp.bfloat16)).astype(jnp.float32)
    weighted = weighted * rescale[..., None] + jnp.einsum("gqk,gkd->gqd", rounded, value_heads)
    return new_max, row_total, weighted


def reference(queries, keys, values, doc_lengths):
    block_rows = TOK_DEV * N_ULY
    group_size = HEADS // KV_HEADS
    query_rows = block_rows * group_size
    starts = (jnp.cumsum(doc_lengths).astype(jnp.int32) - doc_lengths).astype(jnp.int32)
    front_rows = REACH * block_rows
    keys_padded = jnp.pad(keys, ((front_rows, 0), (0, 0)))
    values_padded = jnp.pad(values, ((front_rows, 0), (0, 0)))

    def one_block(block_index):
        first_row = block_index * block_rows
        query_block = lax.dynamic_slice_in_dim(queries, first_row, block_rows, 0)
        grouped = query_block.reshape(block_rows, KV_HEADS, group_size, HEAD_DIM).transpose(1, 0, 2, 3)
        grouped = grouped.reshape(KV_HEADS, query_rows, HEAD_DIM)
        query_pos = first_row + jnp.arange(query_rows, dtype=jnp.int32) // group_size
        query_doc = doc_index(query_pos, starts)
        running = (jnp.full((KV_HEADS, query_rows), MASKED, jnp.float32),
                   jnp.zeros((KV_HEADS, query_rows), jnp.float32),
                   jnp.zeros((KV_HEADS, query_rows, HEAD_DIM), jnp.float32))
        for distance in range(REACH + 1):
            anchor = (block_index - distance).astype(jnp.int32)
            start_row = (front_rows + anchor * block_rows).astype(jnp.int32)
            key_block = lax.dynamic_slice_in_dim(keys_padded, start_row, block_rows, 0)
            value_block = lax.dynamic_slice_in_dim(values_padded, start_row, block_rows, 0)
            if distance == 0:
                running = fold_block(running, grouped, query_pos, query_doc, key_block, value_block, anchor, starts)
            else:
                last_doc = doc_index(jnp.reshape(anchor * block_rows + block_rows - 1, (1,)).astype(jnp.int32), starts)[0]
                needed = (anchor >= 0) & (last_doc == query_doc[0])

                def absorb(state_now, kb=key_block, vb=value_block, source=anchor):
                    return fold_block(state_now, grouped, query_pos, query_doc, kb, vb, source, starts)

                def keep_state(state_now):
                    return state_now

                running = lax.cond(needed, absorb, keep_state, running)
        result = running[2] / running[1][..., None]
        result = result.astype(jnp.bfloat16).reshape(KV_HEADS, block_rows, group_size, HEAD_DIM)
        return result.transpose(1, 0, 2, 3).reshape(block_rows, HEADS * HEAD_DIM)

    blocks_out = lax.map(one_block, jnp.arange(N_BLK, dtype=jnp.int32))
    return blocks_out.reshape(SEQ, HEADS * HEAD_DIM)
```

```python
import functools
import math

import jax
import jax.numpy as jnp
from jax import lax
from jax.experimental import pallas as pl
from jax.experimental.pallas import tpu as pltpu
from jax.sharding import PartitionSpec as P

KV_HEADS = 8
HEAD_DIM = 128
MASKED = -1e30
SCALE = HEAD_DIM ** -0.5 * math.log2(math.e)


def from_behind(value, by):
    size = lax.axis_size("blk")
    return lax.ppermute(value, "blk", [(i, i + by) for i in range(size - by)])


def stage_kernel(back, first, last, lens_ref, q_ref, *refs):
    refs = list(refs)
    k_refs, v_refs = refs[:2], refs[2:4]
    refs = refs[4:]
    if not first:
        stat_in, acc_in = refs[:2]
        refs = refs[2:]
    if last:
        out_ref, bias_ref = refs
    else:
        stat_out, acc_out, bias_ref = refs
    rows = q_ref.shape[0]
    group = q_ref.shape[1] // HEAD_DIM
    width = rows * group
    head = pl.program_id(0)
    blk, uly = lax.axis_index("blk"), lax.axis_index("uly")

    @pl.when(head == 0)
    def _():
        docs = lens_ref.shape[1]
        lens = lens_ref[...].astype(jnp.float32)
        before = lax.broadcasted_iota(jnp.int32, (docs, docs), 1) < lax.broadcasted_iota(jnp.int32, (docs, docs), 0)
        starts = jnp.sum(jnp.where(before, lens, 0.0), axis=1, keepdims=True).astype(jnp.int32)
        lane = lax.broadcasted_iota(jnp.int32, (1, width), 1)
        pos = (2 * blk + uly) * rows + lax.rem(lane, rows)
        low = jnp.max(jnp.where(starts <= pos, starts, 0).astype(jnp.float32), axis=0, keepdims=True).astype(jnp.int32)
        for side in range(2):
            other = uly if side == 0 else 1 - uly
            key = (2 * (blk - back) + other) * rows + lax.broadcasted_iota(jnp.int32, (rows, width), 0)
            allowed = (key >= low) & (key <= pos)
            bias_ref[side * rows : (side + 1) * rows, :] = jnp.where(allowed, 0.0, MASKED)

    q = jnp.concatenate([q_ref[:, j * HEAD_DIM : (j + 1) * HEAD_DIM] for j in range(group)], axis=0)
    k = jnp.concatenate([r[...] for r in k_refs], axis=0)
    v = jnp.concatenate([r[...] for r in v_refs], axis=0)
    s = lax.dot_general(k, q, (((1,), (1,)), ((), ())), preferred_element_type=jnp.float32)
    s = s * SCALE + bias_ref[...]
    m = jnp.max(s, axis=0, keepdims=True)
    if not first:
        m_in = stat_in[0, 0:1, :]
        m = jnp.maximum(m, m_in)
        alpha = jnp.exp2(m_in - m)
    p = jnp.exp2(s - m)
    total = jnp.sum(p, axis=0, keepdims=True)
    acc = lax.dot_general(v, p.astype(jnp.bfloat16), (((0,), (0,)), ((), ())), preferred_element_type=jnp.float32)
    if not first:
        total = total + stat_in[0, 1:2, :] * alpha
        acc = acc + acc_in[0] * alpha
    if last:
        out = (acc / total).T.astype(jnp.bfloat16)
        for j in range(group):
            out_ref[:, j * HEAD_DIM : (j + 1) * HEAD_DIM] = out[j * rows : (j + 1) * rows, :]
    else:
        stat_out[0] = jnp.concatenate([m, total, jnp.zeros((6, width), jnp.float32)], axis=0)
        acc_out[0] = acc


def stage(back, lens, queries, ks, vs, state=None, last=False):
    rows, cols = queries.shape
    per_head = cols // KV_HEADS
    width = rows * per_head // HEAD_DIM
    q_spec = pl.BlockSpec((rows, per_head), lambda g: (0, g))
    kv_spec = pl.BlockSpec((rows, HEAD_DIM), lambda g: (0, g))
    stat_spec = pl.BlockSpec((1, 8, width), lambda g: (g, 0, 0))
    acc_spec = pl.BlockSpec((1, HEAD_DIM, width), lambda g: (g, 0, 0))
    in_specs = [pl.BlockSpec(lens.shape, lambda g: (0, 0)), q_spec] + [kv_spec] * 4
    args = [lens, queries, *ks, *vs]
    if state is not None:
        in_specs += [stat_spec, acc_spec]
        args += list(state)
    if last:
        out_specs = q_spec
        out_shape = jax.ShapeDtypeStruct(queries.shape, queries.dtype)
    else:
        out_specs = (stat_spec, acc_spec)
        out_shape = (
            jax.ShapeDtypeStruct((KV_HEADS, 8, width), jnp.float32),
            jax.ShapeDtypeStruct((KV_HEADS, HEAD_DIM, width), jnp.float32),
        )
    return pl.pallas_call(
        functools.partial(stage_kernel, back, state is None, last),
        grid=(KV_HEADS,),
        in_specs=in_specs,
        out_specs=out_specs,
        out_shape=out_shape,
        scratch_shapes=[pltpu.VMEM((2 * rows, width), jnp.float32)],
        compiler_params=pltpu.CompilerParams(
            dimension_semantics=("arbitrary",), vmem_limit_bytes=24 * 1024 * 1024
        ),
        name=f"stage{back}",
    )(*args)


def local(queries, keys, values, doc_lengths):
    lens = doc_lengths[None, :]
    swap = lambda x, pairs: lax.ppermute(x, "uly", pairs)
    k1, v1 = from_behind(keys, 1), from_behind(values, 1)
    k2, v2 = from_behind(keys, 2), from_behind(values, 2)
    up, both, down = [(0, 1)], [(0, 1), (1, 0)], [(1, 0)]
    k0s, v0s = swap(keys, up), swap(values, up)
    state = stage(0, lens, queries, (keys, k0s), (values, v0s))
    k1s, v1s = swap(k1, both), swap(v1, both)
    state = stage(1, lens, queries, (k1, k1s), (v1, v1s), state)
    k2s, v2s = swap(k2, down), swap(v2, down)
    return stage(2, lens, queries, (k2, k2s), (v2, v2s), state, last=True)


def solution(mesh):
    spec = P(("blk", "uly"), None)
    return jax.shard_map(local, mesh=mesh, in_specs=(spec, spec, spec, P()), out_specs=spec, check_vma=False)
```

```python
import functools
import math

import jax
import jax.numpy as jnp
from jax import lax
from jax.experimental import pallas as pl
from jax.experimental.pallas import tpu as pltpu
from jax.sharding import PartitionSpec as P


KV_HEADS = 8
HEAD_DIM = 128
MASKED = -1e30
SCALE = HEAD_DIM ** -0.5 * math.log2(math.e)
TILE = 256


def from_behind(value, by, sides=(0, 1)):
    size = lax.axis_size("blk")
    pairs = [(2 * i + side, 2 * (i + by) + side) for i in range(size - by) for side in sides]
    return lax.ppermute(value, ("blk", "uly"), pairs)


def attend(q_ref, shards, bias_ref, state_in, state_out=None, out_ref=None, before=None, after=None):
    rows = q_ref.shape[0]
    group = q_ref.shape[1] // HEAD_DIM // KV_HEADS
    width = rows * group
    tile = math.gcd(TILE, width)
    keys = rows * len(shards)
    ones = jnp.ones((16, keys), jnp.bfloat16)
    units = [(g, u) for g in range(KV_HEADS) for u in range(width // tile)]

    def stacked(g):
        return jnp.concatenate([r[:, g * HEAD_DIM : (g + 1) * HEAD_DIM] for r in shards], axis=0)

    def segments(g, u):
        at = u * tile
        while at < (u + 1) * tile:
            j, row = divmod(at, rows)
            take = min(rows - row, (u + 1) * tile - at)
            yield at - u * tile, take, row, (g * group + j) * HEAD_DIM
            at += take

    def scores(g, u):
        if u == 0 and before is not None:
            before(g)
        q = jnp.concatenate([q_ref[row : row + take, col : col + HEAD_DIM] for _, take, row, col in segments(g, u)], axis=0)
        s = lax.dot_general(stacked(g), q, (((1,), (1,)), ((), ())), preferred_element_type=jnp.float32)
        return s * SCALE + bias_ref[:keys, u * tile : (u + 1) * tile]

    ahead = scores(*units[0])
    for i, (g, u) in enumerate(units):
        s = ahead
        if i + 1 < len(units):
            ahead = scores(*units[i + 1])
        if u == 0:
            v = jnp.concatenate([stacked(KV_HEADS + g).T, ones], axis=0)
        cols = slice(u * tile, (u + 1) * tile)
        m = jnp.max(s, axis=0, keepdims=True)
        if state_in is not None:
            stat_in, acc_in = state_in
            m_in = stat_in[g, 0:1, cols]
            m = jnp.maximum(m, m_in)
            alpha = jnp.exp2(m_in - m)
        p = jnp.exp2(s - m).astype(jnp.bfloat16)
        acc = lax.dot_general(v, p, (((1,), (0,)), ((), ())), preferred_element_type=jnp.float32)
        total = acc[HEAD_DIM : HEAD_DIM + 1]
        acc = acc[:HEAD_DIM]
        if state_in is not None:
            total = total + stat_in[g, 1:2, cols] * alpha
            acc = acc + acc_in[g, :, cols] * alpha
        if out_ref is not None:
            out = (acc * (1.0 / total)).astype(jnp.bfloat16).T
            for at, take, row, col in segments(g, u):
                out_ref[row : row + take, col : col + HEAD_DIM] = out[at : at + take]
            if (u + 1) * tile == width and after is not None:
                after(g)
        else:
            stat_out, acc_out = state_out
            stat_out[g, 0:1, cols] = m
            stat_out[g, 1:2, cols] = total
            acc_out[g, :, cols] = acc


def write_bias(bias_ref, at, rows, first_key, low, pos=None):
    width = bias_ref.shape[1]
    key = first_key + lax.broadcasted_iota(jnp.int32, (rows, width), 0)
    allowed = key >= low
    if pos is not None:
        allowed &= key <= pos
    bias_ref[at : at + rows, :] = jnp.where(allowed, 0.0, MASKED)


def load_kernel(keys_hbm, values_hbm, lens_hbm, kv_ref, lens_ref, sems):
    cols = keys_hbm.shape[1]
    copies = [
        pltpu.make_async_copy(keys_hbm, kv_ref.at[:, :cols], sems.at[0]),
        pltpu.make_async_copy(values_hbm, kv_ref.at[:, cols:], sems.at[1]),
        pltpu.make_async_copy(lens_hbm, lens_ref, sems.at[2]),
    ]
    for copy in copies:
        copy.start()
    for copy in copies:
        copy.wait()


def plan_kernel(rows, lens_ref, low_ref, wide_ref, _):
    blk, uly = lax.axis_index("blk"), lax.axis_index("uly")
    docs = lens_ref.shape[1]
    lens = lens_ref[...].astype(jnp.float32)
    here = lax.broadcasted_iota(jnp.int32, (docs, docs), 0)
    there = lax.broadcasted_iota(jnp.int32, (docs, docs), 1)
    starts = jnp.sum(jnp.where(there < here, lens, 0.0), axis=1, keepdims=True).astype(jnp.int32)
    ends = jnp.sum(jnp.where(there <= here, lens, 0.0), axis=1, keepdims=True).astype(jnp.int32)
    reach = 2 * rows * lax.div(ends - 1, 2 * rows) - 3 * rows
    wide_ref[0] = jnp.max(jnp.where(starts < reach, 1.0, 0.0)).astype(jnp.int32)
    lane = lax.broadcasted_iota(jnp.int32, low_ref.shape, 1)
    pos = (2 * blk + uly) * rows + lax.rem(lane, rows)
    low_ref[...] = jnp.max(jnp.where(starts <= pos, starts, 0).astype(jnp.float32), axis=0, keepdims=True).astype(jnp.int32)


def head_copy(src, dst, sems, g):
    cols = src.shape[1] // KV_HEADS
    at = slice(g * cols, (g + 1) * cols)
    return pltpu.make_async_copy(src.at[:, at], dst.at[:, at], sems.at[g])


def own_kernel(q_hbm, low_ref, kv_ref, mate_ref, q_ref, stat_ref, acc_ref, bias_ref, sems):
    for g in range(KV_HEADS):
        head_copy(q_hbm, q_ref, sems, g).start()
    rows = kv_ref.shape[0]
    blk, uly = lax.axis_index("blk"), lax.axis_index("uly")
    low = low_ref[...]
    lane = lax.broadcasted_iota(jnp.int32, low.shape, 1)
    pos = (2 * blk + uly) * rows + lax.rem(lane, rows)
    write_bias(bias_ref, 0, rows, (2 * blk + uly) * rows, low, pos)
    write_bias(bias_ref, rows, rows, (2 * blk + 1 - uly) * rows, low, pos)
    attend(
        q_ref, (kv_ref, mate_ref), bias_ref, None, (stat_ref, acc_ref),
        before=lambda g: head_copy(q_hbm, q_ref, sems, g).wait(),
    )


def near_kernel(side, q_ref, low_ref, kv_ref, stat_in, acc_in, stat_ref, acc_ref, bias_ref):
    rows = kv_ref.shape[0]
    blk, uly = lax.axis_index("blk"), lax.axis_index("uly")
    other = uly if side == 0 else 1 - uly
    write_bias(bias_ref, 0, rows, (2 * blk - 2 + other) * rows, low_ref[...])
    attend(q_ref, (kv_ref,), bias_ref, (stat_in, acc_in), (stat_ref, acc_ref))


def far_kernel(
    wide_ref, q_ref, low_ref, kv_ref, mate_ref, first_hbm, stat_in, acc_in, out_hbm,
    bias_ref, half_ref, first_ref, out_ref, sems, sem,
):
    rows = kv_ref.shape[0]
    blk, uly = lax.axis_index("blk"), lax.axis_index("uly")
    low = low_ref[...]
    write_bias(bias_ref, 0, rows, (2 * blk - 3) * rows, low)
    half_ref[...] = jnp.where(uly == 0, mate_ref[...], kv_ref[...])
    finish = dict(out_ref=out_ref, after=lambda g: head_copy(out_ref, out_hbm, sems, g).start())

    @pl.when(wide_ref[0] == 0)
    def _():
        attend(q_ref, (half_ref,), bias_ref, (stat_in, acc_in), **finish)

    @pl.when(wide_ref[0] != 0)
    def _():
        fetch = pltpu.make_async_copy(first_hbm, first_ref, sem)
        fetch.start()
        write_bias(bias_ref, rows, rows, (2 * blk - 4) * rows, low)
        fetch.wait()
        attend(q_ref, (half_ref, first_ref), bias_ref, (stat_in, acc_in), **finish)

    for g in range(KV_HEADS):
        head_copy(out_ref, out_hbm, sems, g).wait()


VMEM = pl.BlockSpec(memory_space=pltpu.VMEM)
SMEM = pl.BlockSpec(memory_space=pltpu.SMEM)
HBM = pl.BlockSpec(memory_space=pltpu.HBM)


def call(kernel, in_specs, outs, scratch, *args):
    return pl.pallas_call(
        kernel,
        in_specs=in_specs,
        out_specs=tuple(spec for spec, _, _ in outs),
        out_shape=tuple(jax.ShapeDtypeStruct(shape, dtype) for _, shape, dtype in outs),
        scratch_shapes=scratch,
        compiler_params=pltpu.CompilerParams(vmem_limit_bytes=24 * 1024 * 1024),
    )(*args)


def in_hbm(x):
    return pltpu.with_memory_space_constraint(x, pltpu.HBM)


def local(queries, keys, values, doc_lengths):
    rows, cols = queries.shape
    width = rows * cols // KV_HEADS // HEAD_DIM
    docs = doc_lengths.shape[0]
    state = [
        (VMEM, (KV_HEADS, 8, width), jnp.float32),
        (VMEM, (KV_HEADS, HEAD_DIM, width), jnp.float32),
    ]
    bias = pltpu.VMEM((2 * rows, width), jnp.float32)
    half_bias = pltpu.VMEM((rows, width), jnp.float32)
    kv, lens = call(
        load_kernel,
        [HBM] * 3,
        [(VMEM, (rows, 2 * keys.shape[1]), keys.dtype), (VMEM, (1, docs), jnp.int32)],
        [pltpu.SemaphoreType.DMA((3,))],
        in_hbm(keys), in_hbm(values), in_hbm(doc_lengths[None, :]),
    )
    kv1 = from_behind(kv, 1)
    low, wide, spare = call(
        functools.partial(plan_kernel, rows),
        [VMEM],
        [(VMEM, (1, width), jnp.int32), (SMEM, (1,), jnp.int32), (HBM, kv.shape, kv.dtype)],
        [],
        lens,
    )
    first = lax.cond(wide[0] != 0, lambda x, _: from_behind(x, 2, (0,)), lambda _, y: y, kv, spare)
    mate = lax.ppermute(kv, "uly", [(0, 1)])
    q, stat, acc = call(
        own_kernel,
        [HBM, VMEM, VMEM, VMEM],
        [(VMEM, queries.shape, queries.dtype), *state],
        [bias, pltpu.SemaphoreType.DMA((KV_HEADS,))],
        in_hbm(queries), low, kv, mate,
    )
    kv2 = from_behind(kv, 2, (1,))
    mate1 = lax.ppermute(kv1, "uly", [(0, 1), (1, 0)])
    stat, acc = call(functools.partial(near_kernel, 0), [VMEM] * 5, state, [half_bias], q, low, kv1, stat, acc)
    mate2 = lax.ppermute(kv2, "uly", [(1, 0)])
    stat, acc = call(functools.partial(near_kernel, 1), [VMEM] * 5, state, [half_bias], q, low, mate1, stat, acc)
    (out,) = call(
        far_kernel,
        [SMEM] + [VMEM] * 4 + [HBM] + [VMEM] * 2,
        [(HBM, queries.shape, queries.dtype)],
        [
            bias,
            pltpu.VMEM(kv.shape, kv.dtype),
            pltpu.VMEM(kv.shape, kv.dtype),
            pltpu.VMEM(queries.shape, queries.dtype),
            pltpu.SemaphoreType.DMA((KV_HEADS,)),
            pltpu.SemaphoreType.DMA,
        ],
        wide, q, low, kv2, mate2, in_hbm(first), stat, acc,
    )
    return out


def solution(mesh):
    spec = P(("blk", "uly"), None)
    return jax.shard_map(local, mesh=mesh, in_specs=(spec, spec, spec, P()), out_specs=spec, check_vma=False)
```

```python
import functools
import math

import jax
import jax.numpy as jnp
from jax import lax
from jax.experimental import pallas as pl
from jax.experimental.pallas import tpu as pltpu
from jax.sharding import PartitionSpec as P


KV_HEADS = 8
HEAD_DIM = 128
MASKED = -1e30
SCALE = HEAD_DIM ** -0.5 * math.log2(math.e)
TILE = 768


def from_behind(value, by, sides=(0, 1)):
    size = lax.axis_size("blk")
    pairs = [(2 * i + side, 2 * (i + by) + side) for i in range(size - by) for side in sides]
    return lax.ppermute(value, ("blk", "uly"), pairs)


def attend(q_ref, shards, bias_ref, state_in, state_out=None, out_ref=None, before=None, after=None):
    width = q_ref.shape[1]
    rows = shards[0].shape[1]
    tile = math.gcd(TILE, width)
    keys = rows * len(shards)
    ones = jnp.ones((16, keys), jnp.bfloat16)
    units = [(g, u) for g in range(KV_HEADS) for u in range(width // tile)]

    def stacked(g):
        return jnp.concatenate([r[g] for r in shards], axis=0)

    def scores(g, u):
        if u == 0 and before is not None:
            before(g)
        q = q_ref[g, u * tile : (u + 1) * tile, :]
        s = lax.dot_general(stacked(g), q, (((1,), (1,)), ((), ())), preferred_element_type=jnp.float32)
        return s * SCALE + bias_ref[:keys, u * tile : (u + 1) * tile]

    ahead = scores(*units[0])
    for i, (g, u) in enumerate(units):
        s = ahead
        if i + 1 < len(units):
            ahead = scores(*units[i + 1])
        if u == 0:
            v = jnp.concatenate([stacked(KV_HEADS + g).T, ones], axis=0)
        cols = slice(u * tile, (u + 1) * tile)
        m = jnp.max(s, axis=0, keepdims=True)
        if state_in is not None:
            stat_in, acc_in = state_in
            m_in = stat_in[g, 0:1, cols]
            m = jnp.maximum(m, m_in)
            alpha = jnp.exp2(m_in - m)
        p = jnp.exp2(s - m).astype(jnp.bfloat16)
        acc = lax.dot_general(v, p, (((1,), (0,)), ((), ())), preferred_element_type=jnp.float32)
        total = acc[HEAD_DIM : HEAD_DIM + 1]
        acc = acc[:HEAD_DIM]
        if state_in is not None:
            total = total + stat_in[g, 1:2, cols] * alpha
            acc = acc + acc_in[g, :, cols] * alpha
        if out_ref is not None:
            out_ref[g, cols, :] = (acc * (1.0 / total)).astype(jnp.bfloat16).T
            if (u + 1) * tile == width and after is not None:
                after(g)
        else:
            stat_out, acc_out = state_out
            stat_out[g, 0:1, cols] = m
            stat_out[g, 1:2, cols] = total
            acc_out[g, :, cols] = acc


def write_bias(bias_ref, at, rows, first_key, low, pos=None):
    width = bias_ref.shape[1]
    key = first_key + lax.broadcasted_iota(jnp.int32, (rows, width), 0)
    allowed = key >= low
    if pos is not None:
        allowed &= key <= pos
    bias_ref[at : at + rows, :] = jnp.where(allowed, 0.0, MASKED)


def head_copies(flat, heads, sems, g):
    rows = flat.shape[0]
    group = heads.shape[1] // rows
    for j in range(group):
        h = g * group + j
        yield flat.at[:, h * HEAD_DIM : (h + 1) * HEAD_DIM], heads.at[g, j * rows : (j + 1) * rows, :], sems.at[g]


def load_kernel(keys_hbm, values_hbm, lens_hbm, kv_ref, lens_ref, sems):
    copies = [pltpu.make_async_copy(lens_hbm, lens_ref, sems.at[2 * KV_HEADS])]
    for at, flat in ((0, keys_hbm), (KV_HEADS, values_hbm)):
        for g in range(KV_HEADS):
            src = flat.at[:, g * HEAD_DIM : (g + 1) * HEAD_DIM]
            copies.append(pltpu.make_async_copy(src, kv_ref.at[at + g], sems.at[at + g]))
    for copy in copies:
        copy.start()
    for copy in copies:
        copy.wait()


def plan_kernel(rows, lens_ref, low_ref, wide_ref, _):
    blk, uly = lax.axis_index("blk"), lax.axis_index("uly")
    docs = lens_ref.shape[1]
    lens = lens_ref[...].astype(jnp.float32)
    here = lax.broadcasted_iota(jnp.int32, (docs, docs), 0)
    there = lax.broadcasted_iota(jnp.int32, (docs, docs), 1)
    starts = jnp.sum(jnp.where(there < here, lens, 0.0), axis=1, keepdims=True).astype(jnp.int32)
    ends = jnp.sum(jnp.where(there <= here, lens, 0.0), axis=1, keepdims=True).astype(jnp.int32)
    reach = 2 * rows * lax.div(ends - 1, 2 * rows) - 3 * rows
    wide = jnp.max(jnp.where(starts < reach, 1.0, 0.0), axis=0, keepdims=True)
    wide_ref[0] = jnp.max(wide).astype(jnp.int32)
    low_ref[1:2, :] = jnp.broadcast_to(wide.astype(jnp.int32), (1, low_ref.shape[1]))
    lane = lax.broadcasted_iota(jnp.int32, (1, low_ref.shape[1]), 1)
    pos = (2 * blk + uly) * rows + lax.rem(lane, rows)
    low_ref[0:1, :] = jnp.max(jnp.where(starts <= pos, starts, 0).astype(jnp.float32), axis=0, keepdims=True).astype(jnp.int32)


def own_kernel(q_hbm, low_ref, kv_ref, q_ref, stat_ref, acc_ref, bias_ref, sems):
    def fetch(g):
        return [pltpu.make_async_copy(src, dst, sem) for src, dst, sem in head_copies(q_hbm, q_ref, sems, g)]

    def arrived(g):
        for copy in fetch(g):
            copy.wait()

    for g in range(KV_HEADS):
        for copy in fetch(g):
            copy.start()
    rows = kv_ref.shape[1]
    blk, uly = lax.axis_index("blk"), lax.axis_index("uly")
    low = low_ref[0:1, :]
    lane = lax.broadcasted_iota(jnp.int32, low.shape, 1)
    pos = (2 * blk + uly) * rows + lax.rem(lane, rows)
    write_bias(bias_ref, 0, rows, (2 * blk + uly) * rows, low, pos)
    attend(
        q_ref, (kv_ref,), bias_ref, None, (stat_ref, acc_ref),
        before=arrived,
    )


def more_kernel(back, q_ref, low_ref, kv_ref, stat_in, acc_in, stat_ref, acc_ref, bias_ref):
    rows = kv_ref.shape[1]
    blk, uly = lax.axis_index("blk"), lax.axis_index("uly")
    low = low_ref[0:1, :]
    if back == 0:
        lane = lax.broadcasted_iota(jnp.int32, low.shape, 1)
        pos = (2 * blk + uly) * rows + lax.rem(lane, rows)
        write_bias(bias_ref, 0, rows, (2 * blk + 1 - uly) * rows, low, pos)
    else:
        write_bias(bias_ref, 0, rows, (2 * blk - 2 + uly) * rows, low)
    attend(q_ref, (kv_ref,), bias_ref, (stat_in, acc_in), (stat_ref, acc_ref))


def last_kernel(
    q_ref, low_ref, kv2_ref, mate2_ref, mate1_ref, first_hbm, stat_in, acc_in, out_hbm,
    bias_ref, half_ref, first_ref, out_ref, sems, sem,
):
    rows = mate1_ref.shape[1]
    blk, uly = lax.axis_index("blk"), lax.axis_index("uly")
    low = low_ref[0:1, :]
    wide = jnp.max(low_ref[1:2, :HEAD_DIM].astype(jnp.float32)) > 0.0
    write_bias(bias_ref, 0, rows, (2 * blk - 1 - uly) * rows, low)
    write_bias(bias_ref, rows, rows, (2 * blk - 3) * rows, low)
    half_ref[...] = jnp.where(uly == 0, mate2_ref[...], kv2_ref[...])

    def store(g):
        return [pltpu.make_async_copy(src, dst, sem) for dst, src, sem in head_copies(out_hbm, out_ref, sems, g)]

    def done(g):
        for copy in store(g):
            copy.start()

    def finish(*shards):
        attend(q_ref, shards, bias_ref, (stat_in, acc_in), out_ref=out_ref, after=done)

    @pl.when(jnp.logical_not(wide))
    def _():
        finish(mate1_ref, half_ref)

    @pl.when(wide)
    def _():
        fetch = pltpu.make_async_copy(first_hbm, first_ref, sem)
        fetch.start()
        write_bias(bias_ref, 2 * rows, rows, (2 * blk - 4) * rows, low)
        fetch.wait()
        finish(mate1_ref, half_ref, first_ref)

    for g in range(KV_HEADS):
        for copy in store(g):
            copy.wait()


VMEM = pl.BlockSpec(memory_space=pltpu.VMEM)
SMEM = pl.BlockSpec(memory_space=pltpu.SMEM)
HBM = pl.BlockSpec(memory_space=pltpu.HBM)


def call(kernel, in_specs, outs, scratch, *args):
    return pl.pallas_call(
        kernel,
        in_specs=in_specs,
        out_specs=tuple(spec for spec, _, _ in outs),
        out_shape=tuple(jax.ShapeDtypeStruct(shape, dtype) for _, shape, dtype in outs),
        scratch_shapes=scratch,
        compiler_params=pltpu.CompilerParams(vmem_limit_bytes=24 * 1024 * 1024),
    )(*args)


def in_hbm(x):
    return pltpu.with_memory_space_constraint(x, pltpu.HBM)


def local(queries, keys, values, doc_lengths):
    rows, cols = queries.shape
    width = rows * cols // KV_HEADS // HEAD_DIM
    docs = doc_lengths.shape[0]
    heads_shape = (KV_HEADS, width, HEAD_DIM)
    state = [
        (VMEM, (KV_HEADS, 8, width), jnp.float32),
        (VMEM, (KV_HEADS, HEAD_DIM, width), jnp.float32),
    ]

    def bias(shards):
        return pltpu.VMEM((shards * rows, width), jnp.float32)

    kv, lens = call(
        load_kernel,
        [HBM] * 3,
        [(VMEM, (2 * KV_HEADS, rows, HEAD_DIM), keys.dtype), (VMEM, (1, docs), jnp.int32)],
        [pltpu.SemaphoreType.DMA((2 * KV_HEADS + 1,))],
        in_hbm(keys), in_hbm(values), in_hbm(doc_lengths[None, :]),
    )
    kv2 = from_behind(kv, 2, (1,))
    kv1 = from_behind(kv, 1)
    low, wide, spare = call(
        functools.partial(plan_kernel, rows),
        [VMEM],
        [(VMEM, (2, width), jnp.int32), (SMEM, (1,), jnp.int32), (HBM, kv.shape, kv.dtype)],
        [],
        lens,
    )
    first = lax.switch(wide[0], [lambda _, y: y, lambda x, _: from_behind(x, 2, (0,))], kv, spare)
    mate = lax.ppermute(kv, "uly", [(0, 1)])
    q, stat, acc = call(
        own_kernel,
        [HBM, VMEM, VMEM],
        [(VMEM, heads_shape, queries.dtype), *state],
        [bias(1), pltpu.SemaphoreType.DMA((KV_HEADS,))],
        in_hbm(queries), low, kv,
    )
    stat, acc = call(functools.partial(more_kernel, 0), [VMEM] * 5, state, [bias(1)], q, low, mate, stat, acc)
    mate2 = lax.ppermute(kv2, "uly", [(1, 0)])
    mate1 = lax.ppermute(kv1, "uly", [(0, 1), (1, 0)])
    stat, acc = call(functools.partial(more_kernel, 1), [VMEM] * 5, state, [bias(1)], q, low, kv1, stat, acc)
    (out,) = call(
        last_kernel,
        [VMEM] * 5 + [HBM] + [VMEM] * 2,
        [(HBM, queries.shape, queries.dtype)],
        [
            bias(3),
            pltpu.VMEM(kv.shape, kv.dtype),
            pltpu.VMEM(kv.shape, kv.dtype),
            pltpu.VMEM(heads_shape, queries.dtype),
            pltpu.SemaphoreType.DMA((KV_HEADS,)),
            pltpu.SemaphoreType.DMA,
        ],
        q, low, kv2, mate2, mate1, in_hbm(first), stat, acc,
    )
    return out


def solution(mesh):
    spec = P(("blk", "uly"), None)
    return jax.shard_map(local, mesh=mesh, in_specs=(spec, spec, spec, P()), out_specs=spec, check_vma=False)
```

```python
import functools
import math

import jax
import jax.numpy as jnp
from jax import lax
from jax.experimental import pallas as pl
from jax.experimental.pallas import tpu as pltpu
from jax.sharding import PartitionSpec as P


KV_HEADS = 8
HEAD_DIM = 128
MASKED = -1e30
SCALE = HEAD_DIM ** -0.5 * math.log2(math.e)
TILE = 768


def from_behind(value, by, sides=(0, 1)):
    size = lax.axis_size("blk")
    pairs = [(2 * i + side, 2 * (i + by) + side) for i in range(size - by) for side in sides]
    return lax.ppermute(value, ("blk", "uly"), pairs)


def attend(q_ref, shards, bias_ref, state_in, state_out=None, out_ref=None, after=None):
    width = q_ref.shape[1]
    rows = shards[0].shape[1]
    tile = math.gcd(TILE, width)
    keys = rows * len(shards)
    ones = jnp.ones((16, keys), jnp.bfloat16)
    units = [(g, u) for g in range(KV_HEADS) for u in range(width // tile)]

    def stacked(g):
        return jnp.concatenate([r[g] for r in shards], axis=0)

    def scores(g, u):
        q = q_ref[g, u * tile : (u + 1) * tile, :]
        s = lax.dot_general(stacked(g), q, (((1,), (1,)), ((), ())), preferred_element_type=jnp.float32)
        return s * SCALE + bias_ref[:keys, u * tile : (u + 1) * tile]

    if state_in is not None:
        stat_in, acc_in = state_in

    def soften(g, u, s):
        cols = slice(u * tile, (u + 1) * tile)
        m = jnp.max(s, axis=0, keepdims=True)
        alpha = None
        if state_in is not None:
            m_in = stat_in[g, 0:1, cols]
            m = jnp.maximum(m, m_in)
            alpha = jnp.exp2(m_in - m)
        return jnp.exp2(s - m).astype(jnp.bfloat16), m, alpha

    def finish(g, u, p, m, alpha):
        cols = slice(u * tile, (u + 1) * tile)
        v = jnp.concatenate([stacked(KV_HEADS + g).T, ones], axis=0)
        acc = lax.dot_general(v, p, (((1,), (0,)), ((), ())), preferred_element_type=jnp.float32)

        total = acc[HEAD_DIM : HEAD_DIM + 1]
        acc = acc[:HEAD_DIM]
        if state_in is not None:
            total = total + stat_in[g, 1:2, cols] * alpha
            acc = acc + acc_in[g, :, cols] * alpha
        if out_ref is not None:
            out_ref[g, cols, :] = (acc * (1.0 / total)).astype(jnp.bfloat16).T
            if (u + 1) * tile == width and after is not None:
                after(g)
        else:
            stat_out, acc_out = state_out
            stat_out[g, 0:1, cols] = m
            stat_out[g, 1:2, cols] = total
            acc_out[g, :, cols] = acc

    n = len(units)
    s = {0: scores(*units[0])}
    soft = {}
    for i in range(n + 1):
        if i + 1 < n:
            s[i + 1] = scores(*units[i + 1])
        if i < n:
            soft[i] = soften(*units[i], s.pop(i))
        if i >= 1:
            finish(*units[i - 1], *soft.pop(i - 1))


def write_bias(bias_ref, at, rows, first_key, low, pos=None):
    width = bias_ref.shape[1]
    key = first_key + lax.broadcasted_iota(jnp.int32, (rows, width), 0)
    allowed = key >= low
    if pos is not None:
        allowed &= key <= pos
    bias_ref[at : at + rows, :] = jnp.where(allowed, 0.0, MASKED)


def head_copies(flat, heads, sems, g):
    rows = flat.shape[0]
    group = heads.shape[1] // rows
    for j in range(group):
        h = g * group + j
        yield flat.at[:, h * HEAD_DIM : (h + 1) * HEAD_DIM], heads.at[g, j * rows : (j + 1) * rows, :], sems.at[g]


def load_kernel(keys_hbm, values_hbm, lens_hbm, kv_ref, lens_ref, sems):
    copies = [pltpu.make_async_copy(lens_hbm, lens_ref, sems.at[2 * KV_HEADS])]
    for at, flat in ((0, keys_hbm), (KV_HEADS, values_hbm)):
        for g in range(KV_HEADS):
            src = flat.at[:, g * HEAD_DIM : (g + 1) * HEAD_DIM]
            copies.append(pltpu.make_async_copy(src, kv_ref.at[at + g], sems.at[at + g]))
    for copy in copies:
        copy.start()
    for copy in copies:
        copy.wait()


def plan_kernel(rows, lens_ref, low_ref, wide_ref, _):
    blk, uly = lax.axis_index("blk"), lax.axis_index("uly")
    docs = lens_ref.shape[1]
    lens = lens_ref[...].astype(jnp.float32)
    here = lax.broadcasted_iota(jnp.int32, (docs, docs), 0)
    there = lax.broadcasted_iota(jnp.int32, (docs, docs), 1)
    starts = jnp.sum(jnp.where(there < here, lens, 0.0), axis=1, keepdims=True).astype(jnp.int32)
    ends = jnp.sum(jnp.where(there <= here, lens, 0.0), axis=1, keepdims=True).astype(jnp.int32)
    reach = 2 * rows * lax.div(ends - 1, 2 * rows) - 3 * rows
    wide = jnp.max(jnp.where(starts < reach, 1.0, 0.0), axis=0, keepdims=True)
    wide_ref[0] = jnp.max(wide).astype(jnp.int32)
    low_ref[1:2, :] = jnp.broadcast_to(wide.astype(jnp.int32), (1, low_ref.shape[1]))
    lane = lax.broadcasted_iota(jnp.int32, (1, low_ref.shape[1]), 1)
    pos = (2 * blk + uly) * rows + lax.rem(lane, rows)
    low_ref[0:1, :] = jnp.max(jnp.where(starts <= pos, starts, 0).astype(jnp.float32), axis=0, keepdims=True).astype(jnp.int32)


def query_copies(q_hbm, q_ref, sems):
    return [
        pltpu.make_async_copy(src, dst, sem)
        for g in range(KV_HEADS)
        for src, dst, sem in head_copies(q_hbm, q_ref, sems, g)
    ]


def idle_over_far():
    return (lax.axis_index("uly") == 0) | (lax.axis_index("blk") >= lax.axis_size("blk") - 2)


def early_kernel(q_hbm, q_ref, sems):
    @pl.when(idle_over_far())
    def _():
        for copy in query_copies(q_hbm, q_ref, sems):
            copy.start()
        for copy in query_copies(q_hbm, q_ref, sems):
            copy.wait()


def own_kernel(q_hbm, low_ref, kv_ref, _, q_ref, stat_ref, acc_ref, bias_ref, sems):
    blk, uly = lax.axis_index("blk"), lax.axis_index("uly")

    @pl.when(jnp.logical_not(idle_over_far()))
    def _():
        for copy in query_copies(q_hbm, q_ref, sems):
            copy.start()

    rows = kv_ref.shape[1]
    low = low_ref[0:1, :]
    lane = lax.broadcasted_iota(jnp.int32, low.shape, 1)
    pos = (2 * blk + uly) * rows + lax.rem(lane, rows)
    write_bias(bias_ref, 0, rows, (2 * blk + uly) * rows, low, pos)

    @pl.when(jnp.logical_not(idle_over_far()))
    def _():
        for copy in query_copies(q_hbm, q_ref, sems):
            copy.wait()

    attend(q_ref, (kv_ref,), bias_ref, None, (stat_ref, acc_ref))


def more_kernel(back, q_ref, low_ref, kv_ref, stat_in, acc_in, stat_ref, acc_ref, bias_ref):
    rows = kv_ref.shape[1]
    blk, uly = lax.axis_index("blk"), lax.axis_index("uly")
    low = low_ref[0:1, :]
    if back == 0:
        lane = lax.broadcasted_iota(jnp.int32, low.shape, 1)
        pos = (2 * blk + uly) * rows + lax.rem(lane, rows)
        write_bias(bias_ref, 0, rows, (2 * blk + 1 - uly) * rows, low, pos)
    else:
        write_bias(bias_ref, 0, rows, (2 * blk - 2 + uly) * rows, low)
    attend(q_ref, (kv_ref,), bias_ref, (stat_in, acc_in), (stat_ref, acc_ref))


def far_kernel(
    q_ref, low_ref, kv_ref, mate_ref, first_hbm, stat_in, acc_in, stat_ref, acc_ref,
    bias_ref, half_ref, first_ref, sem,
):
    rows = kv_ref.shape[1]
    blk, uly = lax.axis_index("blk"), lax.axis_index("uly")
    low = low_ref[0:1, :]
    wide = jnp.max(low_ref[1:2, :HEAD_DIM].astype(jnp.float32)) > 0.0
    write_bias(bias_ref, 0, rows, (2 * blk - 3) * rows, low)
    half_ref[...] = jnp.where(uly == 0, mate_ref[...], kv_ref[...])

    def fold(*shards):
        attend(q_ref, shards, bias_ref, (stat_in, acc_in), (stat_ref, acc_ref))

    @pl.when(jnp.logical_not(wide))
    def _():
        fold(half_ref)

    @pl.when(wide)
    def _():
        fetch = pltpu.make_async_copy(first_hbm, first_ref, sem)
        fetch.start()
        write_bias(bias_ref, rows, rows, (2 * blk - 4) * rows, low)
        fetch.wait()
        fold(half_ref, first_ref)


def last_kernel(q_ref, low_ref, kv_ref, stat_in, acc_in, out_hbm, bias_ref, out_ref, sems):
    rows = kv_ref.shape[1]
    blk, uly = lax.axis_index("blk"), lax.axis_index("uly")
    write_bias(bias_ref, 0, rows, (2 * blk - 1 - uly) * rows, low_ref[0:1, :])

    def store(g):
        return [pltpu.make_async_copy(src, dst, sem) for dst, src, sem in head_copies(out_hbm, out_ref, sems, g)]

    def done(g):
        for copy in store(g):
            copy.start()

    attend(q_ref, (kv_ref,), bias_ref, (stat_in, acc_in), out_ref=out_ref, after=done)
    for g in range(KV_HEADS):
        for copy in store(g):
            copy.wait()


VMEM = pl.BlockSpec(memory_space=pltpu.VMEM)
SMEM = pl.BlockSpec(memory_space=pltpu.SMEM)
HBM = pl.BlockSpec(memory_space=pltpu.HBM)


def call(kernel, in_specs, outs, scratch, *args, aliases={}):
    return pl.pallas_call(
        kernel,
        in_specs=in_specs,
        out_specs=tuple(spec for spec, _, _ in outs),
        out_shape=tuple(jax.ShapeDtypeStruct(shape, dtype) for _, shape, dtype in outs),
        scratch_shapes=scratch,
        input_output_aliases=aliases,
        compiler_params=pltpu.CompilerParams(vmem_limit_bytes=24 * 1024 * 1024),
    )(*args)


def in_hbm(x):
    return pltpu.with_memory_space_constraint(x, pltpu.HBM)


def local(queries, keys, values, doc_lengths):
    rows, cols = queries.shape
    width = rows * cols // KV_HEADS // HEAD_DIM
    docs = doc_lengths.shape[0]
    heads_shape = (KV_HEADS, width, HEAD_DIM)
    state = [
        (VMEM, (KV_HEADS, 8, width), jnp.float32),
        (VMEM, (KV_HEADS, HEAD_DIM, width), jnp.float32),
    ]

    def bias(shards):
        return pltpu.VMEM((shards * rows, width), jnp.float32)

    kv, lens = call(
        load_kernel,
        [HBM] * 3,
        [(VMEM, (2 * KV_HEADS, rows, HEAD_DIM), keys.dtype), (VMEM, (1, docs), jnp.int32)],
        [pltpu.SemaphoreType.DMA((2 * KV_HEADS + 1,))],
        in_hbm(keys), in_hbm(values), in_hbm(doc_lengths[None, :]),
    )
    kv2 = from_behind(kv, 2, (1,))
    kv1 = from_behind(kv, 1)
    low, wide, spare = call(
        functools.partial(plan_kernel, rows),
        [VMEM],
        [(VMEM, (2, width), jnp.int32), (SMEM, (1,), jnp.int32), (HBM, kv.shape, kv.dtype)],
        [],
        lens,
    )
    (q,) = call(
        early_kernel,
        [HBM],
        [(VMEM, heads_shape, queries.dtype)],
        [pltpu.SemaphoreType.DMA((KV_HEADS,))],
        in_hbm(queries),
    )
    first = lax.switch(wide[0], [lambda _, y: y, lambda x, _: from_behind(x, 2, (0,))], kv, spare)
    mate = lax.ppermute(kv, "uly", [(0, 1)])
    q, stat, acc = call(
        own_kernel,
        [HBM, VMEM, VMEM, VMEM],
        [(VMEM, heads_shape, queries.dtype), *state],
        [bias(1), pltpu.SemaphoreType.DMA((KV_HEADS,))],
        in_hbm(queries), low, kv, q,
        aliases={3: 0},
    )
    stat, acc = call(functools.partial(more_kernel, 0), [VMEM] * 5, state, [bias(1)], q, low, mate, stat, acc)
    mate2 = lax.ppermute(kv2, "uly", [(1, 0)])
    stat, acc = call(
        far_kernel,
        [VMEM] * 4 + [HBM] + [VMEM] * 2,
        state,
        [bias(2), pltpu.VMEM(kv.shape, kv.dtype), pltpu.VMEM(kv.shape, kv.dtype), pltpu.SemaphoreType.DMA],
        q, low, kv2, mate2, in_hbm(first), stat, acc,
    )
    mate1 = lax.ppermute(kv1, "uly", [(0, 1), (1, 0)])
    stat, acc = call(functools.partial(more_kernel, 1), [VMEM] * 5, state, [bias(1)], q, low, kv1, stat, acc)
    (out,) = call(
        last_kernel,
        [VMEM] * 5,
        [(HBM, queries.shape, queries.dtype)],
        [bias(1), pltpu.VMEM(heads_shape, queries.dtype), pltpu.SemaphoreType.DMA((KV_HEADS,))],
        q, low, mate1, stat, acc,
    )
    return out


def solution(mesh):
    spec = P(("blk", "uly"), None)
    return jax.shard_map(local, mesh=mesh, in_specs=(spec, spec, spec, P()), out_specs=spec, check_vma=False)
```

```python
import functools
import math

import jax
import jax.numpy as jnp
from jax import lax
from jax.experimental import pallas as pl
from jax.experimental.pallas import tpu as pltpu
from jax.sharding import PartitionSpec as P


KV_HEADS = 8
HEAD_DIM = 128
MASKED = -1e30
SCALE = HEAD_DIM ** -0.5 * math.log2(math.e)
TILE = 768


def from_behind(value, by, sides=(0, 1)):
    size = lax.axis_size("blk")
    pairs = [(2 * i + side, 2 * (i + by) + side) for i in range(size - by) for side in sides]
    return lax.ppermute(value, ("blk", "uly"), pairs)


def attend(q_ref, shards, bias_ref, state_in, state_out=None, out_ref=None, after=None):
    width = q_ref.shape[1]
    rows = shards[0].shape[1]
    tile = math.gcd(TILE, width)
    keys = rows * len(shards)
    ones = jnp.ones((16, keys), jnp.bfloat16)
    units = [(g, u) for g in range(KV_HEADS) for u in range(width // tile)]

    def stacked(g):
        return jnp.concatenate([r[g] for r in shards], axis=0)

    def scores(g, u):
        q = q_ref[g, u * tile : (u + 1) * tile, :]
        s = lax.dot_general(stacked(g), q, (((1,), (1,)), ((), ())), preferred_element_type=jnp.float32)
        return s * SCALE + bias_ref[:keys, u * tile : (u + 1) * tile]

    if state_in is not None:
        stat_in, acc_in = state_in

    def soften(g, u, s):
        cols = slice(u * tile, (u + 1) * tile)
        m = jnp.max(s, axis=0, keepdims=True)
        alpha = None
        if state_in is not None:
            m_in = stat_in[g, 0:1, cols]
            m = jnp.maximum(m, m_in)
            alpha = jnp.exp2(m_in - m)
        return jnp.exp2(s - m).astype(jnp.bfloat16), m, alpha

    def finish(g, u, p, m, alpha):
        cols = slice(u * tile, (u + 1) * tile)
        v = jnp.concatenate([stacked(KV_HEADS + g).T, ones], axis=0)
        acc = lax.dot_general(v, p, (((1,), (0,)), ((), ())), preferred_element_type=jnp.float32)

        total = acc[HEAD_DIM : HEAD_DIM + 1]
        acc = acc[:HEAD_DIM]
        if state_in is not None:
            total = total + stat_in[g, 1:2, cols] * alpha
            acc = acc + acc_in[g, :, cols] * alpha
        if out_ref is not None:
            out_ref[g, cols, :] = (acc * (1.0 / total)).astype(jnp.bfloat16).T
            if (u + 1) * tile == width and after is not None:
                after(g)
        else:
            stat_out, acc_out = state_out
            stat_out[g, 0:1, cols] = m
            stat_out[g, 1:2, cols] = total
            acc_out[g, :, cols] = acc

    n = len(units)
    s = {0: scores(*units[0])}
    soft = {}
    for i in range(n + 1):
        if i + 1 < n:
            s[i + 1] = scores(*units[i + 1])
        if i < n:
            soft[i] = soften(*units[i], s.pop(i))
        if i >= 1:
            finish(*units[i - 1], *soft.pop(i - 1))


def write_bias(bias_ref, at, rows, first_key, low, pos=None):
    width = bias_ref.shape[1]
    key = first_key + lax.broadcasted_iota(jnp.int32, (rows, width), 0)
    allowed = key >= low
    if pos is not None:
        allowed &= key <= pos
    bias_ref[at : at + rows, :] = jnp.where(allowed, 0.0, MASKED)


def head_copies(flat, heads, sems, g):
    rows = flat.shape[0]
    group = heads.shape[1] // rows
    for j in range(group):
        h = g * group + j
        yield flat.at[:, h * HEAD_DIM : (h + 1) * HEAD_DIM], heads.at[g, j * rows : (j + 1) * rows, :], sems.at[g]


def load_kernel(keys_hbm, values_hbm, lens_hbm, kv_ref, lens_ref, sems):
    copies = [pltpu.make_async_copy(lens_hbm, lens_ref, sems.at[2 * KV_HEADS])]
    for at, flat in ((0, keys_hbm), (KV_HEADS, values_hbm)):
        for g in range(KV_HEADS):
            src = flat.at[:, g * HEAD_DIM : (g + 1) * HEAD_DIM]
            copies.append(pltpu.make_async_copy(src, kv_ref.at[at + g], sems.at[at + g]))
    for i, copy in enumerate(copies):
        copy.start(priority=i % 2)
    for copy in copies:
        copy.wait()


def plan_kernel(rows, lens_ref, low_ref, wide_ref, _):
    blk, uly = lax.axis_index("blk"), lax.axis_index("uly")
    docs = lens_ref.shape[1]
    lens = lens_ref[...].astype(jnp.float32)
    here = lax.broadcasted_iota(jnp.int32, (docs, docs), 0)
    there = lax.broadcasted_iota(jnp.int32, (docs, docs), 1)
    starts = jnp.sum(jnp.where(there < here, lens, 0.0), axis=1, keepdims=True).astype(jnp.int32)
    ends = jnp.sum(jnp.where(there <= here, lens, 0.0), axis=1, keepdims=True).astype(jnp.int32)
    reach = 2 * rows * lax.div(ends - 1, 2 * rows) - 3 * rows
    wide = jnp.max(jnp.where(starts < reach, 1.0, 0.0), axis=0, keepdims=True)
    wide_ref[0] = jnp.max(wide).astype(jnp.int32)
    low_ref[1:2, :] = jnp.broadcast_to(wide.astype(jnp.int32), (1, low_ref.shape[1]))
    lane = lax.broadcasted_iota(jnp.int32, (1, low_ref.shape[1]), 1)
    pos = (2 * blk + uly) * rows + lax.rem(lane, rows)
    low_ref[0:1, :] = jnp.max(jnp.where(starts <= pos, starts, 0).astype(jnp.float32), axis=0, keepdims=True).astype(jnp.int32)


def query_copies(q_hbm, q_ref, sems):
    return [
        pltpu.make_async_copy(src, dst, sem)
        for g in range(KV_HEADS)
        for src, dst, sem in head_copies(q_hbm, q_ref, sems, g)
    ]


def idle_over_far():
    return (lax.axis_index("uly") == 0) | (lax.axis_index("blk") >= lax.axis_size("blk") - 2)


def early_kernel(q_hbm, q_ref, sems):
    @pl.when(idle_over_far())
    def _():
        for copy in query_copies(q_hbm, q_ref, sems):
            copy.start()
        for copy in query_copies(q_hbm, q_ref, sems):
            copy.wait()


def own_kernel(q_hbm, low_ref, kv_ref, _, q_ref, stat_ref, acc_ref, bias_ref, sems):
    blk, uly = lax.axis_index("blk"), lax.axis_index("uly")

    @pl.when(jnp.logical_not(idle_over_far()))
    def _():
        for copy in query_copies(q_hbm, q_ref, sems):
            copy.start()

    rows = kv_ref.shape[1]
    low = low_ref[0:1, :]
    lane = lax.broadcasted_iota(jnp.int32, low.shape, 1)
    pos = (2 * blk + uly) * rows + lax.rem(lane, rows)
    write_bias(bias_ref, 0, rows, (2 * blk + uly) * rows, low, pos)

    @pl.when(jnp.logical_not(idle_over_far()))
    def _():
        for copy in query_copies(q_hbm, q_ref, sems):
            copy.wait()

    attend(q_ref, (kv_ref,), bias_ref, None, (stat_ref, acc_ref))


def reached(low_ref, first_key, rows):
    return low_ref[0:1, :HEAD_DIM][0, 0] < first_key + rows


def more_kernel(back, q_ref, low_ref, kv_ref, stat_in, acc_in, stat_ref, acc_ref, bias_ref):
    rows = kv_ref.shape[1]
    blk, uly = lax.axis_index("blk"), lax.axis_index("uly")
    if back == 0:
        first_key = (2 * blk + 1 - uly) * rows
        needed = (uly == 1) & reached(low_ref, first_key, rows)
    else:
        first_key = (2 * blk - 2 + uly) * rows
        needed = reached(low_ref, first_key, rows)

    @pl.when(needed)
    def _():
        write_bias(bias_ref, 0, rows, first_key, low_ref[0:1, :])
        attend(q_ref, (kv_ref,), bias_ref, (stat_in, acc_in), (stat_ref, acc_ref))

    @pl.when(jnp.logical_not(needed))
    def _():
        for g in range(KV_HEADS):
            stat_ref[g] = stat_in[g]
            acc_ref[g] = acc_in[g]


def far_kernel(
    q_ref, low_ref, kv_ref, mate_ref, first_hbm, stat_in, acc_in, stat_ref, acc_ref,
    bias_ref, half_ref, first_ref, sem,
):
    rows = kv_ref.shape[1]
    blk, uly = lax.axis_index("blk"), lax.axis_index("uly")
    low = low_ref[0:1, :]
    wide = jnp.max(low_ref[1:2, :HEAD_DIM].astype(jnp.float32)) > 0.0
    write_bias(bias_ref, 0, rows, (2 * blk - 3) * rows, low)
    half_ref[...] = jnp.where(uly == 0, mate_ref[...], kv_ref[...])

    def fold(*shards):
        attend(q_ref, shards, bias_ref, (stat_in, acc_in), (stat_ref, acc_ref))

    @pl.when(jnp.logical_not(wide))
    def _():
        fold(half_ref)

    @pl.when(wide)
    def _():
        fetch = pltpu.make_async_copy(first_hbm, first_ref, sem)
        fetch.start()
        write_bias(bias_ref, rows, rows, (2 * blk - 4) * rows, low)
        fetch.wait()
        fold(half_ref, first_ref)


def last_kernel(q_ref, low_ref, kv_ref, stat_in, acc_in, out_hbm, bias_ref, out_ref, sems):
    rows = kv_ref.shape[1]
    blk, uly = lax.axis_index("blk"), lax.axis_index("uly")
    first_key = (2 * blk - 1 - uly) * rows
    needed = reached(low_ref, first_key, rows)

    def store(g):
        return [pltpu.make_async_copy(src, dst, sem) for dst, src, sem in head_copies(out_hbm, out_ref, sems, g)]

    def done(g):
        for copy in store(g):
            copy.start()

    @pl.when(needed)
    def _():
        write_bias(bias_ref, 0, rows, first_key, low_ref[0:1, :])
        attend(q_ref, (kv_ref,), bias_ref, (stat_in, acc_in), out_ref=out_ref, after=done)

    @pl.when(jnp.logical_not(needed))
    def _():
        for g in range(KV_HEADS):
            out_ref[g] = (acc_in[g] * (1.0 / stat_in[g, 1:2, :])).astype(jnp.bfloat16).T
            done(g)

    for g in range(KV_HEADS):
        for copy in store(g):
            copy.wait()


VMEM = pl.BlockSpec(memory_space=pltpu.VMEM)
SMEM = pl.BlockSpec(memory_space=pltpu.SMEM)
HBM = pl.BlockSpec(memory_space=pltpu.HBM)


def call(kernel, in_specs, outs, scratch, *args, aliases={}):
    return pl.pallas_call(
        kernel,
        in_specs=in_specs,
        out_specs=tuple(spec for spec, _, _ in outs),
        out_shape=tuple(jax.ShapeDtypeStruct(shape, dtype) for _, shape, dtype in outs),
        scratch_shapes=scratch,
        input_output_aliases=aliases,
        compiler_params=pltpu.CompilerParams(vmem_limit_bytes=24 * 1024 * 1024),
    )(*args)


def in_hbm(x):
    return pltpu.with_memory_space_constraint(x, pltpu.HBM)


def local(queries, keys, values, doc_lengths):
    rows, cols = queries.shape
    width = rows * cols // KV_HEADS // HEAD_DIM
    docs = doc_lengths.shape[0]
    heads_shape = (KV_HEADS, width, HEAD_DIM)
    state = [
        (VMEM, (KV_HEADS, 8, width), jnp.float32),
        (VMEM, (KV_HEADS, HEAD_DIM, width), jnp.float32),
    ]

    def bias(shards):
        return pltpu.VMEM((shards * rows, width), jnp.float32)

    kv, lens = call(
        load_kernel,
        [HBM] * 3,
        [(VMEM, (2 * KV_HEADS, rows, HEAD_DIM), keys.dtype), (VMEM, (1, docs), jnp.int32)],
        [pltpu.SemaphoreType.DMA((2 * KV_HEADS + 1,))],
        in_hbm(keys), in_hbm(values), in_hbm(doc_lengths[None, :]),
    )
    kv2 = from_behind(kv, 2, (1,))
    kv1 = from_behind(kv, 1)
    low, wide, spare = call(
        functools.partial(plan_kernel, rows),
        [VMEM],
        [(VMEM, (2, width), jnp.int32), (SMEM, (1,), jnp.int32), (HBM, kv.shape, kv.dtype)],
        [],
        lens,
    )
    (q,) = call(
        early_kernel,
        [HBM],
        [(VMEM, heads_shape, queries.dtype)],
        [pltpu.SemaphoreType.DMA((KV_HEADS,))],
        in_hbm(queries),
    )
    first = lax.switch(wide[0], [lambda _, y: y, lambda x, _: from_behind(x, 2, (0,))], kv, spare)
    mate = lax.ppermute(kv, "uly", [(0, 1)])
    q, stat, acc = call(
        own_kernel,
        [HBM, VMEM, VMEM, VMEM],
        [(VMEM, heads_shape, queries.dtype), *state],
        [bias(1), pltpu.SemaphoreType.DMA((KV_HEADS,))],
        in_hbm(queries), low, kv, q,
        aliases={3: 0},
    )
    stat, acc = call(functools.partial(more_kernel, 0), [VMEM] * 5, state, [bias(1)], q, low, mate, stat, acc)
    mate2 = lax.ppermute(kv2, "uly", [(1, 0)])
    stat, acc = call(
        far_kernel,
        [VMEM] * 4 + [HBM] + [VMEM] * 2,
        state,
        [bias(2), pltpu.VMEM(kv.shape, kv.dtype), pltpu.VMEM(kv.shape, kv.dtype), pltpu.SemaphoreType.DMA],
        q, low, kv2, mate2, in_hbm(first), stat, acc,
    )
    mate1 = lax.ppermute(kv1, "uly", [(0, 1), (1, 0)])
    stat, acc = call(functools.partial(more_kernel, 1), [VMEM] * 5, state, [bias(1)], q, low, kv1, stat, acc)
    (out,) = call(
        last_kernel,
        [VMEM] * 5,
        [(HBM, queries.shape, queries.dtype)],
        [bias(1), pltpu.VMEM(heads_shape, queries.dtype), pltpu.SemaphoreType.DMA((KV_HEADS,))],
        q, low, mate1, stat, acc,
    )
    return out


def solution(mesh):
    spec = P(("blk", "uly"), None)
    return jax.shard_map(local, mesh=mesh, in_specs=(spec, spec, spec, P()), out_specs=spec, check_vma=False)
```
